32 devices in a mesh: groups: 2 (over y), expert: 4 (over z), mp: 4 (over x, core).
Axes of the slice: x: 2, y: 2, z: 4, core: 2. Of those that a mesh axis runs over, the one named last changes fastest.
Arguments:
- tokens: bfloat16 [6144, 1024], P(('groups', 'expert'), 'mp'), parts along dimension 0, may hold values from -60 to 60
- gain: float32 [1024], replicated, may hold values from 0.1 to 1.9
- w_res_in: bfloat16 [1024, 4096], P(None, 'mp'), may hold values from -0.1875 to 0.1875
- w_res_out: bfloat16 [4096, 1024], P('mp'), may hold values from -0.09375 to 0.09375
- w_exp_in: bfloat16 [4, 1024, 4096], P('expert', None, 'mp'), may hold values from -0.1875 to 0.1875
- w_exp_out: bfloat16 [4, 4096, 1024], P('expert', 'mp'), may hold values from -0.09375 to 0.09375
- expert_of: int32 [6144], P(('groups', 'expert')), parts along dimension 0, may hold values from 0 to 3
- slot_of: int32 [6144], P(('groups', 'expert')), parts along dimension 0, may hold values from -1 to 239, as said below
- gate_prob: float32 [6144], P(('groups', 'expert')), parts along dimension 0, may hold values from 0.2 to 1
Outputs:
- layer_out: bfloat16 [6144, 1024], P(('groups', 'expert'), 'mp'), parts along dimension 0
The draws below stay inside these ranges and needn't reach their ends.
There are 2 independent parts, one for each index of `groups`. The reference program is written for one: setup_inputs(seed, part) draws one part's arguments, and reference() takes and returns one part's arrays. A program takes and returns all parts, laid end to end along the dimension named above; an argument that names none is the same for every part. Nothing has to cross between parts.
Inputs may be any that keep to these rules, and one draw needn't show every extreme that they name: slot_of[t] is the number of earlier tokens of t's aligned block of 768 tokens with the same expert_of, or -1 where that number is 240 or more. In every draw one expert has more than 240 tokens in every aligned block.
All inputs are finite; a program needn't handle non-finite values.
Results may differ from the reference program's by a relative error of at most 0.014.
Values may be sent and summed in bfloat16 or wider, within the bound.
A program may use at most 64 MiB of HBM per device.

```python
import math
import jax
import jax.numpy as jnp
from jax import lax

D = 1024
FE = 4096
FR = 4096
TOK_DEV = 768
EXPERTS = 4
TOKENS = 3072
CAP = 240
N_EXPERT = 4
N_MP = 4


def draw_tokens(key, part):
    mixed = jax.random.fold_in(key, 11)
    key_base, key_rows, key_cols = jax.random.split(mixed, 3)
    base = jnp.clip(jax.random.normal(key_base, (TOKENS, D), jnp.float32), -5.5, 5.5)
    row_scale = jnp.exp(jax.random.uniform(key_rows, (TOKENS, 1), jnp.float32) * math.log(10.0))
    col_scale = jnp.exp(jax.random.uniform(key_cols, (1, D), jnp.float32) * math.log(10.0))
    return (base * row_scale * col_scale / 10.0).astype(jnp.bfloat16)


def shuffle(subkey):
    return jax.random.permutation(subkey, TOK_DEV)


def routing_pair(key):
    mixed = jax.random.fold_in(key, 5)
    key_base, key_hot, key_perm = jax.random.split(mixed, 3)
    blocks = TOKENS // TOK_DEV
    base = jax.random.randint(key_base, (blocks, TOK_DEV), 0, EXPERTS)
    hottest = jax.random.randint(key_hot, (1, 1), 0, EXPERTS)
    order = jax.vmap(shuffle)(jax.random.split(key_perm, blocks))
    chosen = order < CAP + 2
    expert_ids = jnp.where(chosen, hottest, base).astype(jnp.int32)
    same = expert_ids[:, :, None] == expert_ids[:, None, :]
    index = jnp.arange(TOK_DEV, dtype=jnp.int32)
    earlier = index[None, :] < index[:, None]
    rank = jnp.sum(jnp.logical_and(same, earlier[None]).astype(jnp.int32), axis=2)
    slots = jnp.where(rank < CAP, rank, -1).astype(jnp.int32)
    return (expert_ids.reshape(TOKENS), slots.reshape(TOKENS))


def draw_expert_of(key, part):
    return routing_pair(key)[0]


def draw_slot_of(key, part):
    return routing_pair(key)[1]


def level_of(own_key, extent, shards, low, largest):
    loudness = 1.0
    for axis_at, parts in shards:
        heights = jax.random.uniform(jax.random.fold_in(jax.random.fold_in(own_key, 6), axis_at), (parts,), jnp.float32, low / len(shards), largest / len(shards))
        loudness = loudness * jnp.repeat(jnp.exp(heights), extent[axis_at] // parts).reshape((-1,) + (1,) * (len(extent) - 1 - axis_at))
    return loudness


def gaussian(stream_key, dims, deviation, most, shards=(), kind=jnp.bfloat16):
    result = jax.random.normal(stream_key, dims, jnp.float32) * deviation
    if len(shards) > 0:
        result = level_of(stream_key, dims, shards, -0.22, 0.18) * result
    return jnp.clip(result, min=-most, max=most).astype(kind)


def setup_inputs(seed: int = 0, part: int = 0) -> dict:
    arg_keys = jax.random.split(jax.random.key(seed), 10)
    part_keys = jax.random.split(jax.random.fold_in(arg_keys[9], part), 10)
    return {
        "tokens": draw_tokens(jax.random.fold_in(jax.random.fold_in(arg_keys[9], part), 71), part),
        "gain": jnp.clip(1.0 + 0.18 * jax.random.normal(arg_keys[1], (D,), jnp.float32), 0.1, 1.9),
        "w_res_in": gaussian(arg_keys[2], (D, FR), D ** -0.5, 0.1875, ((1, 4),)),
        "w_res_out": gaussian(arg_keys[3], (FR, D), FR ** -0.5, 0.09375, ((0, 4),)),
        "w_exp_in": gaussian(arg_keys[4], (EXPERTS, D, FE), D ** -0.5, 0.1875, ((0, 4), (2, 4))),
        "w_exp_out": gaussian(arg_keys[5], (EXPERTS, FE, D), FE ** -0.5, 0.09375, ((0, 4), (1, 4))),
        "expert_of": draw_expert_of(jax.random.fold_in(jax.random.fold_in(arg_keys[9], part), 71), part),
        "slot_of": draw_slot_of(jax.random.fold_in(jax.random.fold_in(arg_keys[9], part), 71), part),
        "gate_prob": jnp.clip(jnp.exp(math.log(1.0) - 1.609438 * jax.random.uniform(part_keys[8], (TOKENS,), jnp.float32) ** level_of(part_keys[8], (TOKENS,), ((0, 4),), -0.2, 0.2)), 0.2, 1.0),
    }


def rms_rows(tokens, gain):
    values = tokens.astype(jnp.float32)
    inverse = lax.rsqrt(lax.optimization_barrier(jnp.mean(values * values, axis=-1, keepdims=True)) + 1e-05)
    return (values * inverse * gain.astype(jnp.float32)).astype(jnp.bfloat16)

def block_sums(hidden, w_out):
    width = hidden.shape[1] // N_MP
    total = jnp.zeros((hidden.shape[0], w_out.shape[1]), jnp.float32)
    for block in range(N_MP):
        part = jnp.dot(hidden[:, block * width:(block + 1) * width], w_out[block * width:(block + 1) * width], preferred_element_type=jnp.float32)
        total = total + part.astype(jnp.bfloat16).astype(jnp.float32)
    return total

def reference(tokens, gain, w_res_in, w_res_out, w_exp_in, w_exp_out, expert_of, slot_of, gate_prob):
    normed = rms_rows(tokens, gain)
    res_hidden = jax.nn.gelu(jnp.dot(normed, w_res_in, preferred_element_type=jnp.float32)).astype(jnp.bfloat16)
    res_sum = block_sums(res_hidden, w_res_out)
    blocks = N_EXPERT
    position = jnp.arange(TOKENS, dtype=jnp.int32)
    block_of = position // TOK_DEV
    slots_all = EXPERTS * blocks * CAP
    destination = jnp.where(slot_of >= 0, expert_of * (blocks * CAP) + block_of * CAP + slot_of, slots_all).astype(jnp.int32)
    buffer = jnp.zeros((slots_all + 1, D), jnp.bfloat16).at[destination].set(normed)
    expert_in = buffer[:slots_all].reshape(EXPERTS, blocks * CAP, D)

    def one_expert(item):
        rows, w_in, w_out = item
        hidden = jax.nn.gelu(jnp.dot(rows, w_in, preferred_element_type=jnp.float32)).astype(jnp.bfloat16)
        return block_sums(hidden, w_out).astype(jnp.bfloat16)
    expert_out = lax.map(one_expert, (expert_in, w_exp_in, w_exp_out))
    flat_rows = jnp.concatenate([expert_out.reshape(slots_all, D), jnp.zeros((1, D), jnp.bfloat16)], axis=0)
    moe_value = flat_rows[destination].astype(jnp.float32)
    return (res_sum + gate_prob[:, None] * moe_value).astype(jnp.bfloat16)
```

```python
import functools

import jax
import jax.numpy as jnp
from jax import lax
from jax.experimental import pallas as pl
from jax.experimental.pallas import tpu as pltpu
from jax.sharding import PartitionSpec as P


def rms_rows(tokens, gain):
    values = tokens.astype(jnp.float32)
    inverse = lax.rsqrt(jnp.mean(values * values, axis=-1, keepdims=True) + 1e-05)
    return (values * inverse * gain).astype(jnp.bfloat16)


def per_device(
    tokens, gain, w_res_in, w_res_out, w_exp_in, w_exp_out, expert_of, slot_of, gate_prob
):
    full_rows = lax.all_gather(tokens, "mp", axis=1, tiled=True)
    normed = rms_rows(full_rows, gain)
    res_hidden = jax.nn.gelu(jnp.dot(normed, w_res_in, preferred_element_type=jnp.float32)).astype(
        jnp.bfloat16
    )
    res_part = jnp.dot(res_hidden, w_res_out, preferred_element_type=jnp.float32)
    row_count = expert_of.shape[0]
    experts = lax.axis_size("expert")
    capacity = max(2, 5 * row_count // (4 * experts))
    feat_width = tokens.shape[1]
    slot_id = jnp.where(slot_of >= 0, expert_of * capacity + slot_of, -1)
    slot_index = jnp.arange(experts * capacity, dtype=jnp.int32)
    send_table = (slot_index[:, None] == slot_id[None, :]).astype(jnp.bfloat16)
    take_table = (slot_id[:, None] == slot_index[None, :]).astype(jnp.bfloat16)
    local_in = w_exp_in[0]
    local_out = w_exp_out[0]
    mp_index = lax.axis_index("mp")
    own_slice = lax.dynamic_slice_in_dim(normed, mp_index * feat_width, feat_width, 1)
    outgoing = jnp.dot(send_table, own_slice, preferred_element_type=jnp.float32).astype(
        jnp.bfloat16
    )
    incoming = lax.all_to_all(
        outgoing.reshape(experts, capacity, feat_width),
        "expert",
        split_axis=0,
        concat_axis=0,
        tiled=True,
    )
    piece = lax.all_gather(incoming, "mp", axis=2, tiled=True)
    flat_piece = piece.reshape(-1, piece.shape[2])
    preact = jnp.dot(flat_piece, local_in, preferred_element_type=jnp.float32)
    exp_hidden = jax.nn.gelu(preact).astype(jnp.bfloat16)
    exp_part = jnp.dot(exp_hidden, local_out, preferred_element_type=jnp.float32)
    gate_column = gate_prob[:, None]
    summed = lax.psum_scatter(exp_part.astype(jnp.bfloat16), "mp", scatter_dimension=1, tiled=True)
    returned = lax.all_to_all(
        summed.reshape(experts, capacity, feat_width),
        "expert",
        split_axis=0,
        concat_axis=0,
        tiled=True,
    )
    moe_value = jnp.dot(
        take_table,
        returned.reshape(experts * capacity, feat_width),
        preferred_element_type=jnp.float32,
    )
    res_sum = lax.psum_scatter(
        res_part.astype(jnp.bfloat16), "mp", scatter_dimension=1, tiled=True
    ).astype(jnp.float32)
    return (res_sum + gate_column * moe_value).astype(jnp.bfloat16)


MESH = pl.DeviceIdType.MESH
F32 = jnp.float32
BF16 = jnp.bfloat16


def dot(a, b):
    return jnp.dot(a, b, preferred_element_type=F32)


def gelu_rows(rows, w_ref):
    return jax.nn.gelu(dot(rows, w_ref[...])).astype(BF16)


def fused_kernel(
    spans, pieces, tokens_h, gain_h, w_ri_h, w_ro_h, w_ei_h, w_eo_h, expert_h, slot_h, gate_h, out,
    expert_v, slot_v, gate_v, gain, w_ri, w_ro, w_ei, w_eo, tok, normed, res_hid, rows_raw, out_rows, out_rows2,
    rows_near, rows_far, hid_near, hid, own_part, de_send, de_recv, e_keep, pair_send, pair_recv, xf_send, xf_recv,
    zf_send, zf_recv, dt_send, dt_recv, t_keep, xt_send, xt_recv, gate_col, id_col, load_sem, send_sem, recv_sem,
):
    shards, count, width = tok.shape
    cap = out_rows.shape[1]
    me = lax.axis_index("mp")
    z = lax.axis_index("expert")
    core = lax.rem(me, 2)
    over = lax.rem(me + 2, 4)
    mate = me + 1 - 2 * core
    cross = lax.rem(mate + 2, 4)
    pair = z + 1 - 2 * lax.rem(z, 2)
    far = (lax.rem(z + 2, 4), 3 - z)
    to_over, to_mate, to_pair = {"mp": over}, {"mp": mate}, {"expert": pair}
    to_far = ({"expert": far[0]}, {"expert": far[1]})

    barrier = pltpu.get_barrier_semaphore()
    for dest in (to_over, to_mate, to_pair, to_far[0], to_far[1]):
        pl.semaphore_signal(barrier, inc=1, device_id=dest, device_id_type=MESH)

    loads = []
    for k, (src, dst) in enumerate((
        (expert_h, expert_v), (slot_h, slot_v), (tokens_h, tok.at[me]), (gate_h, gate_v), (gain_h, gain),
        (w_ri_h, w_ri), (w_ei_h.at[0], w_ei), (w_eo_h.at[0], w_eo), (w_ro_h, w_ro),
    )):
        load = pltpu.make_async_copy(src, dst, load_sem.at[k])
        load.start()
        loads.append(load)

    sent = []

    def send(src, dst, dest):
        k = len(sent)
        copy = pltpu.make_async_remote_copy(
            src_ref=src, dst_ref=dst, send_sem=send_sem.at[k], recv_sem=recv_sem.at[k],
            device_id=dest, device_id_type=MESH,
        )
        copy.start()
        sent.append(copy)
        return copy

    def pass_on(ref, dest):
        return send(ref, ref, dest)

    def send_table(e):
        base = (e * cap).astype(F32)
        return jnp.where(slot_rows + base == ids, 1.0, 0.0).astype(BF16)

    def take_table(e):
        base = (e * cap).astype(F32)
        return jnp.where(slot_cols + base == id_col[:, :1], 1.0, 0.0).astype(BF16)

    def shard_cols(s):
        return pl.ds(pl.multiple_of(s * width, width), width)

    def normalize(load, dst, rows):
        total = 0.0
        for s in range(shards):
            v = load(s).astype(F32)
            total = total + jnp.sum(v * v, axis=-1, keepdims=True)
        inverse = lax.rsqrt(total / (shards * width) + 1e-05)
        for s in range(shards):
            cols = slice(s * width, (s + 1) * width)
            dst[rows, cols] = (load(s).astype(F32) * inverse * gain[:, cols]).astype(BF16)

    with jax.named_scope("entry"):
        loads[0].wait()
        loads[1].wait()
        expert_row = expert_v[...].reshape(1, count)
        slot_row = slot_v[...].reshape(1, count)
        ids = jnp.where(slot_row >= 0, expert_row * cap + slot_row, -1).astype(F32)
        slot_rows = lax.broadcasted_iota(jnp.int32, (cap, count), 0).astype(F32)
        slot_cols = lax.broadcasted_iota(jnp.int32, (count, cap), 1).astype(F32)
        loads[2].wait()
        for k, e in enumerate((pair, far[0], far[1])):
            out_rows[k] = dot(send_table(e), tok[me]).astype(BF16)
    with jax.named_scope("barrier"):
        pl.semaphore_wait(barrier, 5)

    tok_over = [send(tok.at[me, r], tok.at[me, r], to_over) for r in spans]
    tok_mate = pass_on(tok.at[me], to_mate)
    z_in = [None, None]

    def far_send(f):
        z_in[f] = [send(out_rows.at[f + 1, r], rows_raw.at[me, f + 1, r], to_far[f]) for r in pieces]

    far_send(0)
    pair_in = send(out_rows.at[0], rows_raw.at[me, 0], to_pair)
    far_send(1)
    with jax.named_scope("columns"):
        id_col[...] = jnp.broadcast_to(ids, (128, count)).T
        loads[3].wait()
        gate_col[...] = jnp.broadcast_to(gate_v[...].reshape(1, count), (128, count)).T
        for k in range(4, 9):
            loads[k].wait()

    tok_cross = []

    def relay(h):
        with jax.named_scope(f"relay{h}"):
            tok_over[h].wait_recv()
            tok_cross.append(pass_on(tok.at[over, spans[h]], to_mate))

    def residual(h):
        r = spans[h]
        with jax.named_scope(f"reswait{h}"):
            tok_cross[h].wait_recv()
        with jax.named_scope(f"residual{h}"):
            normalize(lambda s: tok[s, r], normed, r)
            res_hid[r] = gelu_rows(normed[r], w_ri)

    x_in, d_in, d_in2 = ([], []), ([], []), ([], [])

    def far_in(f, p):
        with jax.named_scope(f"farin{f}{p}"):
            z_in[f][p].wait_recv()
            piece = rows_raw.at[me, f + 1, pieces[p]]
            x_in[f].append(pass_on(piece, to_over))
            d_in[f].append(pass_on(piece, to_mate))

    def far_cross(f, p):
        with jax.named_scope(f"farcross{f}{p}"):
            x_in[f][p].wait_recv()
            d_in2[f].append(pass_on(rows_raw.at[over, f + 1, pieces[p]], to_mate))

    de = {}

    def give(e, j, s, hid_ref):
        de_send[j, e] = dot(hid_ref[...], w_eo[:, shard_cols(s)]).astype(BF16)
        de[j, e] = send(de_send.at[j, e], de_recv.at[j, e], to_mate)

    def keep(e, j, s, hid_ref):
        e_keep[j, e] = dot(hid_ref[...], w_eo[:, shard_cols(s)])

    def chip_part(e, j):
        de[j, e].wait_recv()
        return e_keep[j, e] + de_recv[j, e].astype(F32)

    def expert_rows(e, hid_ref):
        with jax.named_scope(f"expert{e}"):
            normalize(lambda s: rows_raw[s, e], rows_far.at[e], slice(0, cap))
            hid_ref[...] = gelu_rows(rows_far[e], w_ei)
            give(e, 1, cross, hid_ref)
            keep(e, 1, over, hid_ref)
            give(e, 0, mate, hid_ref)
            keep(e, 0, me, hid_ref)

    last = len(pieces)
    relay(0)
    tok_mate.wait_recv()
    residual(0)
    for p in range(last):
        far_in(0, p)
    for h in range(1, len(spans)):
        relay(h)
    with jax.named_scope("pairsend"):
        out_rows2[...] = dot(send_table(pair), tok[over]).astype(BF16)
        pair_in2 = send(out_rows2, rows_raw.at[over, 0], to_pair)
    for p in range(last - 1):
        far_in(1, p)
    for h in range(1, len(spans)):
        residual(h)
    far_in(1, last - 1)
    for p in range(last):
        far_cross(0, p)
    with jax.named_scope("ownfirst"):
        rows_near[...] = dot(send_table(z), normed[...]).astype(BF16)
        hid_near[...] = gelu_rows(rows_near[...], w_ei)
    with jax.named_scope("farwait0"):
        for p in range(last):
            d_in[0][p].wait_recv()
            d_in2[0][p].wait_recv()
    expert_rows(1, hid.at[1])
    with jax.named_scope("pairrelay"):
        pair_in.wait_recv()
        pair_d = pass_on(rows_raw.at[me, 0], to_mate)
        pair_in2.wait_recv()
        pair_d2 = pass_on(rows_raw.at[over, 0], to_mate)
    for p in range(last):
        far_cross(1, p)
    xf, zf = [], []

    def far_out(f):
        with jax.named_scope(f"farout{f}"):
            xf_send[f] = chip_part(f + 1, 1).astype(BF16)
            xf.append(send(xf_send.at[f], xf_recv.at[f], to_over))

    def far_home(f):
        with jax.named_scope(f"farhome{f}"):
            xf[f].wait_recv()
            zf_send[f] = (chip_part(f + 1, 0) + xf_recv[f].astype(F32)).astype(BF16)
            zf.append(send(zf_send.at[f], zf_recv.at[f], to_far[f]))

    pair_out = {}

    def pair_home(j):
        with jax.named_scope(f"pairhome{j}"):
            pair_send[j] = chip_part(0, j).astype(BF16)
            pair_out[j] = send(pair_send.at[j], pair_recv.at[j], to_pair)

    far_out(0)
    with jax.named_scope("pairwait"):
        pair_d.wait_recv()
        pair_d2.wait_recv()
    expert_rows(0, hid.at[0])
    with jax.named_scope("farwait1"):
        for p in range(last):
            d_in[1][p].wait_recv()
            d_in2[1][p].wait_recv()
    expert_rows(2, hid.at[2])
    pair_home(1)
    far_out(1)
    far_home(0)
    pair_home(0)
    with jax.named_scope("ownsecond"):
        for s in range(shards):
            own_part[s] = dot(hid_near[...], w_eo[:, s * width:(s + 1) * width]).astype(BF16)
        own_take = take_table(z)
        pair_take = take_table(pair)
    dt = {}

    def token_part(s):
        return dot(res_hid[...], w_ro[:, shard_cols(s)]) + gate_col[:, :1] * dot(own_take, own_part[s])

    def token_give(j, s):
        dt_send[j] = token_part(s).astype(BF16)
        dt[j] = send(dt_send.at[j], dt_recv.at[j], to_mate)

    def chip_sum(j):
        pair_out[j].wait_recv()
        dt[j].wait_recv()
        return t_keep[j] + dt_recv[j].astype(F32) + gate_col[:, :1] * dot(pair_take, pair_recv[j])

    with jax.named_scope("tokens1"):
        token_give(1, cross)
        t_keep[1] = token_part(over)
    with jax.named_scope("tokensend"):
        xt_send[...] = chip_sum(1).astype(BF16)
        xt = send(xt_send, xt_recv, to_over)
    with jax.named_scope("tokens0"):
        token_give(0, mate)
        t_keep[0] = token_part(me)
    far_home(1)
    with jax.named_scope("tokenkeep"):
        t_keep[0] = chip_sum(0)
    for f in range(2):
        with jax.named_scope(f"fartake{f}"):
            far_take = take_table(far[f])
            zf[f].wait_recv()
            t_keep[0] = t_keep[0] + gate_col[:, :1] * dot(far_take, zf_recv[f])
    with jax.named_scope("final"):
        xt.wait_recv()
        out[...] = (t_keep[0] + xt_recv[...].astype(F32)).astype(BF16)
        for copy in sent:
            copy.wait_send()


def split_rows(rows, parts):
    step = -(-rows // (16 * parts)) * 16
    return tuple(slice(lo, min(lo + step, rows)) for lo in range(0, rows, step))


def fused(tokens, gain, w_res_in, w_res_out, w_exp_in, w_exp_out, expert_of, slot_of, gate_prob):
    count, width = tokens.shape
    shards = lax.axis_size("mp")
    experts = lax.axis_size("expert")
    cap = max(2, 5 * count // (4 * experts))
    model, hidden = w_res_in.shape
    exp_hidden = w_exp_in.shape[2]
    vmem, hbm = pl.BlockSpec(memory_space=pltpu.VMEM), pl.BlockSpec(memory_space=pltpu.HBM)
    buf = lambda *shape: pltpu.VMEM(shape, BF16)
    wide = lambda *shape: pltpu.VMEM(shape, F32)
    spans, pieces = split_rows(count, 2), split_rows(cap, 2)
    copies = 20 + 2 * len(spans) + 8 * len(pieces)
    args = (
        tokens, gain[None, :], w_res_in, w_res_out, w_exp_in, w_exp_out, expert_of, slot_of, gate_prob,
    )
    return pl.pallas_call(
        functools.partial(fused_kernel, spans, pieces),
        out_shape=jax.ShapeDtypeStruct((count, width), BF16),
        in_specs=[hbm] * len(args),
        out_specs=vmem,
        scratch_shapes=[
            pltpu.VMEM((count,), jnp.int32), pltpu.VMEM((count,), jnp.int32), wide(count), wide(1, model),
            buf(model, hidden), buf(hidden, model), buf(model, exp_hidden), buf(exp_hidden, model),
            buf(shards, count, width), buf(count, model), buf(count, hidden),
            buf(shards, 3, cap, width), buf(3, cap, width), buf(cap, width),
            buf(cap, model), buf(3, cap, model), buf(cap, exp_hidden), buf(3, cap, exp_hidden),
            buf(shards, cap, width), buf(2, 3, cap, width), buf(2, 3, cap, width), wide(2, 3, cap, width),
            buf(2, cap, width), buf(2, cap, width), buf(2, cap, width), buf(2, cap, width),
            buf(2, cap, width), buf(2, cap, width),
            buf(2, count, width), buf(2, count, width), wide(2, count, width),
            buf(count, width), buf(count, width), wide(count, 128), wide(count, 128),
            pltpu.SemaphoreType.DMA((9,)), pltpu.SemaphoreType.DMA((copies,)), pltpu.SemaphoreType.DMA((copies,)),
        ],
        name="fused_layer",
        compiler_params=pltpu.CompilerParams(
            collective_id=0, has_side_effects=True, vmem_limit_bytes=50 * 1024 * 1024
        ),
    )(*(pltpu.with_memory_space_constraint(a, pltpu.HBM) for a in args))


def pick(mesh):
    if mesh.shape["mp"] == 4 and mesh.shape["expert"] == 4:
        return fused
    return per_device


def solution(mesh):
    return jax.shard_map(
        pick(mesh),
        mesh=mesh,
        in_specs=(
            P(("groups", "expert"), "mp"),
            P(),
            P(None, "mp"),
            P("mp", None),
            P("expert", None, "mp"),
            P("expert", "mp", None),
            P(("groups", "expert")),
            P(("groups", "expert")),
            P(("groups", "expert")),
        ),
        out_specs=P(("groups", "expert"), "mp"),
        check_vma=False,
    )
```

```python
import functools

import jax
import jax.numpy as jnp
from jax import lax
from jax.experimental import pallas as pl
from jax.experimental.pallas import tpu as pltpu
from jax.sharding import PartitionSpec as P


def rms_rows(tokens, gain):
    values = tokens.astype(jnp.float32)
    inverse = lax.rsqrt(jnp.mean(values * values, axis=-1, keepdims=True) + 1e-05)
    return (values * inverse * gain).astype(jnp.bfloat16)


def per_device(
    tokens, gain, w_res_in, w_res_out, w_exp_in, w_exp_out, expert_of, slot_of, gate_prob
):
    full_rows = lax.all_gather(tokens, "mp", axis=1, tiled=True)
    normed = rms_rows(full_rows, gain)
    res_hidden = jax.nn.gelu(jnp.dot(normed, w_res_in, preferred_element_type=jnp.float32)).astype(
        jnp.bfloat16
    )
    res_part = jnp.dot(res_hidden, w_res_out, preferred_element_type=jnp.float32)
    row_count = expert_of.shape[0]
    experts = lax.axis_size("expert")
    capacity = max(2, 5 * row_count // (4 * experts))
    feat_width = tokens.shape[1]
    slot_id = jnp.where(slot_of >= 0, expert_of * capacity + slot_of, -1)
    slot_index = jnp.arange(experts * capacity, dtype=jnp.int32)
    send_table = (slot_index[:, None] == slot_id[None, :]).astype(jnp.bfloat16)
    take_table = (slot_id[:, None] == slot_index[None, :]).astype(jnp.bfloat16)
    local_in = w_exp_in[0]
    local_out = w_exp_out[0]
    mp_index = lax.axis_index("mp")
    own_slice = lax.dynamic_slice_in_dim(normed, mp_index * feat_width, feat_width, 1)
    outgoing = jnp.dot(send_table, own_slice, preferred_element_type=jnp.float32).astype(
        jnp.bfloat16
    )
    incoming = lax.all_to_all(
        outgoing.reshape(experts, capacity, feat_width),
        "expert",
        split_axis=0,
        concat_axis=0,
        tiled=True,
    )
    piece = lax.all_gather(incoming, "mp", axis=2, tiled=True)
    flat_piece = piece.reshape(-1, piece.shape[2])
    preact = jnp.dot(flat_piece, local_in, preferred_element_type=jnp.float32)
    exp_hidden = jax.nn.gelu(preact).astype(jnp.bfloat16)
    exp_part = jnp.dot(exp_hidden, local_out, preferred_element_type=jnp.float32)
    gate_column = gate_prob[:, None]
    summed = lax.psum_scatter(exp_part.astype(jnp.bfloat16), "mp", scatter_dimension=1, tiled=True)
    returned = lax.all_to_all(
        summed.reshape(experts, capacity, feat_width),
        "expert",
        split_axis=0,
        concat_axis=0,
        tiled=True,
    )
    moe_value = jnp.dot(
        take_table,
        returned.reshape(experts * capacity, feat_width),
        preferred_element_type=jnp.float32,
    )
    res_sum = lax.psum_scatter(
        res_part.astype(jnp.bfloat16), "mp", scatter_dimension=1, tiled=True
    ).astype(jnp.float32)
    return (res_sum + gate_column * moe_value).astype(jnp.bfloat16)


MESH = pl.DeviceIdType.MESH
F32 = jnp.float32
BF16 = jnp.bfloat16


def dot(a, b):
    return jnp.dot(a, b, preferred_element_type=F32)


def twice_gelu(x):
    bent = x * (0.7978845608028654 + 0.035677408136300125 * (x * x))
    return (x + x * jnp.tanh(bent)).astype(BF16)


def fused_kernel(
    spans, pieces, cap, tokens_h, gain_h, w_ri_h, w_ro_h, w_ei_h, w_eo_h, expert_h, slot_h, gate_h, out,
    expert_v, slot_v, gate_v, gain, w_ri, w_ro, w_ei, w_eo, tok, normed, res_hid, rows_raw, out_rows, out_rows2,
    rows_own, hid_own, rows_far, hid, part, de_recv, pair_send, pair_recv, xf_send, xf_recv, zf_send, zf_recv,
    back, take, slot_gate, tpart, dt_recv, t_keep, xt_send, xt_recv, id_col, load_sem, send_sem, recv_sem,
):
    shards, count, width = tok.shape
    padded = take.shape[2]
    hidden = res_hid.shape[1] - padded
    me = lax.axis_index("mp")
    z = lax.axis_index("expert")
    core = lax.rem(me, 2)
    chip = me // 2
    over = lax.rem(me + 2, 4)
    mate = me + 1 - 2 * core
    cross = lax.rem(mate + 2, 4)
    pair = z + 1 - 2 * lax.rem(z, 2)
    far = (lax.rem(z + 2, 4), 3 - z)
    to_over, to_mate, to_pair = {"mp": over}, {"mp": mate}, {"expert": pair}
    to_far = ({"expert": far[0]}, {"expert": far[1]})

    barrier = pltpu.get_barrier_semaphore()
    for dest in (to_over, to_mate, to_pair, to_far[0], to_far[1]):
        pl.semaphore_signal(barrier, inc=1, device_id=dest, device_id_type=MESH)

    loads = []
    for k, (src, dst) in enumerate((
        (expert_h, expert_v), (slot_h, slot_v), (tokens_h, tok.at[me]), (gate_h, gate_v), (gain_h, gain),
        (w_ri_h, w_ri), (w_ei_h.at[0], w_ei), (w_eo_h.at[0], w_eo), (w_ro_h, w_ro.at[:hidden]),
    )):
        load = pltpu.make_async_copy(src, dst, load_sem.at[k])
        load.start()
        loads.append(load)

    sent = []

    def send(src, dst, dest):
        k = len(sent)
        copy = pltpu.make_async_remote_copy(
            src_ref=src, dst_ref=dst, send_sem=send_sem.at[k], recv_sem=recv_sem.at[k],
            device_id=dest, device_id_type=MESH,
        )
        copy.start()
        sent.append(copy)
        return copy

    def pass_on(ref, dest):
        return send(ref, ref, dest)

    def send_table(e):
        base = (e * cap).astype(F32)
        return jnp.where(slot_rows + base == ids, 1.0, 0.0).astype(BF16)

    def chip_cols(j):
        block = chip if j == 0 else 1 - chip
        return pl.ds(pl.multiple_of(block * 2 * width, 2 * width), 2 * width)

    def normalize(load, dst, rows):
        total = 0.0
        for s in range(shards):
            v = load(s).astype(F32)
            total = total + jnp.sum(v * v, axis=-1, keepdims=True)
        inverse = lax.rsqrt(total / (shards * width) + 1e-05)
        for s in range(shards):
            cols = slice(s * width, (s + 1) * width)
            dst[rows, cols] = (load(s).astype(F32) * inverse * gain[:, cols]).astype(BF16)

    z_in = [None, None]

    def far_send(f):
        out_rows[f + 1] = dot(send_table(far[f]), tok[me]).astype(BF16)
        z_in[f] = [send(out_rows.at[f + 1, r], rows_raw.at[me, f + 1, r], to_far[f]) for r in pieces]

    with jax.named_scope("entry"):
        loads[0].wait()
        loads[1].wait()
        expert_row = expert_v[...].reshape(1, count)
        slot_row = slot_v[...].reshape(1, count)
        ids = jnp.where(slot_row >= 0, expert_row * cap + slot_row, -1).astype(F32)
        slot_rows = lax.broadcasted_iota(jnp.int32, (cap, count), 0).astype(F32)
        loads[2].wait()
    with jax.named_scope("barrier"):
        pl.semaphore_wait(barrier, 5)
    with jax.named_scope("dispatch"):
        tok_over = [pass_on(tok.at[me, r], to_over) for r in spans]
        tok_mate = pass_on(tok.at[me], to_mate)
        far_send(0)
        out_rows[0] = dot(send_table(pair), tok[me]).astype(BF16)
        pair_in = send(out_rows.at[0], rows_raw.at[me, 0], to_pair)
        far_send(1)
    with jax.named_scope("columns"):
        loads[3].wait()
        gate_row = gate_v[...].reshape(1, count)
        id_col[...] = jnp.broadcast_to(ids, (128, count)).T
        lanes = lax.broadcasted_iota(jnp.int32, (count, 128), 1).astype(F32)
        for k, e in enumerate((pair, far[0], far[1], z)):
            base = (e * cap).astype(F32)
            gates = jnp.sum(jnp.where(slot_rows + base == ids, gate_row, 0.0), axis=1, keepdims=True)
            slot_gate[k] = jnp.broadcast_to(gates, (cap, 128))
            for lo in range(0, padded, 128):
                hit = jnp.where(lanes + (base + lo) == id_col[...], 1.0, 0.0).astype(BF16)
                if k < 3:
                    take[k, :, lo:lo + 128] = hit
                else:
                    res_hid[:, hidden + lo:hidden + lo + 128] = hit
        back[:, cap:, :] = jnp.zeros((4, padded - cap, width), BF16)
        for k in range(4, 9):
            loads[k].wait()
        w_ro[hidden + cap:, :] = jnp.zeros((padded - cap, shards * width), BF16)

    def gated(rows, k):
        scale = slot_gate[k]
        return (rows * jnp.concatenate([scale] * (rows.shape[1] // 128), axis=1)).astype(BF16)

    tok_cross = []

    def relay(h):
        with jax.named_scope(f"relay{h}"):
            tok_over[h].wait_recv()
            tok_cross.append(pass_on(tok.at[over, spans[h]], to_mate))

    def residual(h):
        r = spans[h]
        with jax.named_scope(f"reswait{h}"):
            tok_cross[h].wait_recv()
        with jax.named_scope(f"residual{h}"):
            normalize(lambda s: tok[s, r], normed, r)
            res_hid[r, :hidden] = twice_gelu(dot(normed[r], w_ri[...]))

    x_in, d_in, d_in2 = ([], []), ([], []), ([], [])

    def far_in(f, p):
        with jax.named_scope(f"farin{f}{p}"):
            z_in[f][p].wait_recv()
            piece = rows_raw.at[me, f + 1, pieces[p]]
            x_in[f].append(pass_on(piece, to_over))
            d_in[f].append(pass_on(piece, to_mate))

    def far_cross(f, p):
        with jax.named_scope(f"farcross{f}{p}"):
            x_in[f][p].wait_recv()
            d_in2[f].append(pass_on(rows_raw.at[over, f + 1, pieces[p]], to_mate))

    de = {}

    def chip_part(e, j):
        de[j, e].wait_recv()
        return part[e, over if j else me].astype(F32) + de_recv[j, e].astype(F32)

    def expert_first(e):
        with jax.named_scope(f"first{e}"):
            normalize(lambda s: rows_raw[s, e], rows_far.at[e], slice(0, cap))
            hid[e] = twice_gelu(dot(rows_far[e], w_ei[...]))

    def expert_second(e):
        with jax.named_scope(f"second{e}"):
            full = dot(hid[e], w_eo[...])
            for s in range(shards):
                part[e, s] = full[:, s * width:(s + 1) * width].astype(BF16)
            for j, s in ((1, cross), (0, mate)):
                de[j, e] = send(part.at[e, s], de_recv.at[j, e], to_mate)

    xf, zf = ([], []), ([], [])

    def far_out(f):
        with jax.named_scope(f"farout{f}"):
            xf_send[f] = chip_part(f + 1, 1).astype(BF16)
            for r in pieces:
                xf[f].append(send(xf_send.at[f, r], xf_recv.at[f, r], to_over))

    def far_home(f, p):
        r = pieces[p]
        with jax.named_scope(f"farhome{f}{p}"):
            if p == 0:
                de[0, f + 1].wait_recv()
            xf[f][p].wait_recv()
            own = part[f + 1, me, r].astype(F32) + de_recv[0, f + 1, r].astype(F32)
            zf_send[f, r] = (own + xf_recv[f, r].astype(F32)).astype(BF16)
            zf[f].append(send(zf_send.at[f, r], zf_recv.at[f, r], to_far[f]))

    pair_out = {}

    def pair_home(j):
        with jax.named_scope(f"pairhome{j}"):
            pair_send[j] = chip_part(0, j).astype(BF16)
            pair_out[j] = [send(pair_send.at[j, :, c], pair_recv.at[j, :, c], to_pair) for c in lanes]

    dt = ([], [])

    def token_part(j, r):
        with jax.named_scope(f"tokens{j}"):
            both = dot(res_hid[r], w_ro[:, chip_cols(j)])
            for c in range(2):
                tpart[j, c, r] = both[:, c * width:(c + 1) * width].astype(BF16)
            dt[j].append(send(tpart.at[j, 1 - core, r], dt_recv.at[j, r], to_mate))

    def chip_sum(j, c):
        back[j, :cap, c] = gated(pair_recv[j, :, c].astype(F32), 0)
        return dot(take[0], back[j, :, c]) + (tpart[j, core, :, c].astype(F32) + dt_recv[j, :, c].astype(F32))

    def far_wait(f):
        with jax.named_scope(f"farwait{f}"):
            for p in range(last):
                d_in[f][p].wait_recv()
                d_in2[f][p].wait_recv()

    lanes = tuple(slice(lo, lo + 128) for lo in range(0, width, 128))
    last = len(pieces)
    halves = (slice(0, count // 2), slice(count // 2, count))
    tail = len(spans) - 1
    relay(0)
    tok_mate.wait_recv()
    far_in(0, 0)
    for h in range(1, tail):
        relay(h)
        if h == 1:
            for p in range(1, last):
                far_in(0, p)
        residual(h - 1)
    relay(tail)
    with jax.named_scope("pairsend"):
        out_rows2[...] = dot(send_table(pair), tok[over]).astype(BF16)
        pair_in2 = send(out_rows2, rows_raw.at[over, 0], to_pair)
    far_in(1, 0)
    residual(tail - 1)
    for p in range(1, last):
        far_in(1, p)
    for p in range(last):
        far_cross(0, p)
    residual(tail)
    with jax.named_scope("pairrelay"):
        pair_in.wait_recv()
        pair_d = pass_on(rows_raw.at[me, 0], to_mate)
    with jax.named_scope("ownfirst"):
        rows_own[...] = dot(send_table(z), normed[...]).astype(BF16)
        hid_own[...] = twice_gelu(dot(rows_own[...], w_ei[...]))
    with jax.named_scope("pairrelay2"):
        pair_in2.wait_recv()
        pair_d2 = pass_on(rows_raw.at[over, 0], to_mate)
    far_wait(0)
    expert_first(1)
    for p in range(last):
        far_cross(1, p)
    expert_second(1)
    with jax.named_scope("pairwait"):
        pair_d.wait_recv()
        pair_d2.wait_recv()
    expert_first(0)
    expert_second(0)
    far_out(0)
    far_wait(1)
    expert_first(2)
    pair_home(1)
    expert_second(2)
    with jax.named_scope("ownsecond"):
        w_ro[hidden:hidden + cap, :] = gated(dot(hid_own[...], w_eo[...]), 3)
    token_part(1, halves[0])
    far_home(0, 0)
    far_out(1)
    token_part(1, halves[1])
    for p in range(1, last):
        far_home(0, p)
    pair_home(0)
    xt = []
    for k, c in enumerate(lanes):
        with jax.named_scope(f"tokensend{k}"):
            if k == 0:
                for copy in dt[1]:
                    copy.wait_recv()
            pair_out[1][k].wait_recv()
            xt_send[:, c] = chip_sum(1, c).astype(BF16)
            xt.append(send(xt_send.at[:, c], xt_recv.at[:, c], to_over))
    for r in halves:
        token_part(0, r)
    for p in range(last):
        far_home(1, p)
    with jax.named_scope("tokenkeep"):
        for copy in dt[0]:
            copy.wait_recv()
        for k, c in enumerate(lanes):
            pair_out[0][k].wait_recv()
            t_keep[:, c] = chip_sum(0, c)
    for f in range(2):
        with jax.named_scope(f"fartake{f}"):
            for copy in zf[f]:
                copy.wait_recv()
            back[f + 2, :cap] = gated(zf_recv[f].astype(F32), f + 1)
            t_keep[...] = t_keep[...] + dot(take[f + 1], back[f + 2])
    for k, c in enumerate(lanes):
        with jax.named_scope(f"final{k}"):
            xt[k].wait_recv()
            out[:, c] = ((t_keep[:, c] + xt_recv[:, c].astype(F32)) * 0.5).astype(BF16)
    with jax.named_scope("drain"):
        for copy in sent:
            copy.wait_send()


def split_rows(rows, parts):
    step = -(-rows // (16 * parts)) * 16
    return tuple(slice(lo, min(lo + step, rows)) for lo in range(0, rows, step))


def fused(tokens, gain, w_res_in, w_res_out, w_exp_in, w_exp_out, expert_of, slot_of, gate_prob):
    count, width = tokens.shape
    shards = lax.axis_size("mp")
    experts = lax.axis_size("expert")
    cap = max(2, 5 * count // (4 * experts))
    padded = -(-cap // 128) * 128
    model, hidden = w_res_in.shape
    exp_hidden = w_exp_in.shape[2]
    vmem, hbm = pl.BlockSpec(memory_space=pltpu.VMEM), pl.BlockSpec(memory_space=pltpu.HBM)
    buf = lambda *shape: pltpu.VMEM(shape, BF16)
    wide = lambda *shape: pltpu.VMEM(shape, F32)
    spans, pieces = split_rows(count, 4), split_rows(cap, 2)
    copies = 15 + 3 * (width // 128) + 2 * len(spans) + 12 * len(pieces)
    args = (
        tokens, gain[None, :], w_res_in, w_res_out, w_exp_in, w_exp_out, expert_of, slot_of, gate_prob,
    )
    return pl.pallas_call(
        functools.partial(fused_kernel, spans, pieces, cap),
        out_shape=jax.ShapeDtypeStruct((count, width), BF16),
        in_specs=[hbm] * len(args),
        out_specs=vmem,
        scratch_shapes=[
            pltpu.VMEM((count,), jnp.int32), pltpu.VMEM((count,), jnp.int32), wide(count), wide(1, model),
            buf(model, hidden), buf(hidden + padded, model), buf(model, exp_hidden), buf(exp_hidden, model),
            buf(shards, count, width), buf(count, model), buf(count, hidden + padded),
            buf(shards, 3, cap, width), buf(3, cap, width), buf(cap, width),
            buf(cap, model), buf(cap, exp_hidden), buf(3, cap, model), buf(3, cap, exp_hidden),
            buf(3, shards, cap, width), buf(2, 3, cap, width),
            buf(2, cap, width), buf(2, cap, width), buf(2, cap, width), buf(2, cap, width),
            buf(2, cap, width), buf(2, cap, width),
            buf(4, padded, width), buf(3, count, padded), wide(4, cap, 128),
            buf(2, 2, count, width), buf(2, count, width), wide(count, width),
            buf(count, width), buf(count, width), wide(count, 128),
            pltpu.SemaphoreType.DMA((9,)), pltpu.SemaphoreType.DMA((copies,)), pltpu.SemaphoreType.DMA((copies,)),
        ],
        name="fused_layer",
        compiler_params=pltpu.CompilerParams(
            collective_id=0, has_side_effects=True, vmem_limit_bytes=50 * 1024 * 1024
        ),
    )(*(pltpu.with_memory_space_constraint(a, pltpu.HBM) for a in args))


def pick(mesh):
    if mesh.shape["mp"] == 4 and mesh.shape["expert"] == 4:
        return fused
    return per_device


def solution(mesh):
    return jax.shard_map(
        pick(mesh),
        mesh=mesh,
        in_specs=(
            P(("groups", "expert"), "mp"),
            P(),
            P(None, "mp"),
            P("mp", None),
            P("expert", None, "mp"),
            P("expert", "mp", None),
            P(("groups", "expert")),
            P(("groups", "expert")),
            P(("groups", "expert")),
        ),
        out_specs=P(("groups", "expert"), "mp"),
        check_vma=False,
    )
```

```python
import functools

import jax
import jax.numpy as jnp
from jax import lax
from jax.experimental import pallas as pl
from jax.experimental.pallas import tpu as pltpu
from jax.sharding import PartitionSpec as P


def rms_rows(tokens, gain):
    values = tokens.astype(jnp.float32)
    inverse = lax.rsqrt(jnp.mean(values * values, axis=-1, keepdims=True) + 1e-05)
    return (values * inverse * gain).astype(jnp.bfloat16)


def per_device(
    tokens, gain, w_res_in, w_res_out, w_exp_in, w_exp_out, expert_of, slot_of, gate_prob
):
    full_rows = lax.all_gather(tokens, "mp", axis=1, tiled=True)
    normed = rms_rows(full_rows, gain)
    res_hidden = jax.nn.gelu(jnp.dot(normed, w_res_in, preferred_element_type=jnp.float32)).astype(
        jnp.bfloat16
    )
    res_part = jnp.dot(res_hidden, w_res_out, preferred_element_type=jnp.float32)
    row_count = expert_of.shape[0]
    experts = lax.axis_size("expert")
    capacity = max(2, 5 * row_count // (4 * experts))
    feat_width = tokens.shape[1]
    slot_id = jnp.where(slot_of >= 0, expert_of * capacity + slot_of, -1)
    slot_index = jnp.arange(experts * capacity, dtype=jnp.int32)
    send_table = (slot_index[:, None] == slot_id[None, :]).astype(jnp.bfloat16)
    take_table = (slot_id[:, None] == slot_index[None, :]).astype(jnp.bfloat16)
    local_in = w_exp_in[0]
    local_out = w_exp_out[0]
    mp_index = lax.axis_index("mp")
    own_slice = lax.dynamic_slice_in_dim(normed, mp_index * feat_width, feat_width, 1)
    outgoing = jnp.dot(send_table, own_slice, preferred_element_type=jnp.float32).astype(
        jnp.bfloat16
    )
    incoming = lax.all_to_all(
        outgoing.reshape(experts, capacity, feat_width),
        "expert",
        split_axis=0,
        concat_axis=0,
        tiled=True,
    )
    piece = lax.all_gather(incoming, "mp", axis=2, tiled=True)
    flat_piece = piece.reshape(-1, piece.shape[2])
    preact = jnp.dot(flat_piece, local_in, preferred_element_type=jnp.float32)
    exp_hidden = jax.nn.gelu(preact).astype(jnp.bfloat16)
    exp_part = jnp.dot(exp_hidden, local_out, preferred_element_type=jnp.float32)
    gate_column = gate_prob[:, None]
    summed = lax.psum_scatter(exp_part.astype(jnp.bfloat16), "mp", scatter_dimension=1, tiled=True)
    returned = lax.all_to_all(
        summed.reshape(experts, capacity, feat_width),
        "expert",
        split_axis=0,
        concat_axis=0,
        tiled=True,
    )
    moe_value = jnp.dot(
        take_table,
        returned.reshape(experts * capacity, feat_width),
        preferred_element_type=jnp.float32,
    )
    res_sum = lax.psum_scatter(
        res_part.astype(jnp.bfloat16), "mp", scatter_dimension=1, tiled=True
    ).astype(jnp.float32)
    return (res_sum + gate_column * moe_value).astype(jnp.bfloat16)


MESH = pl.DeviceIdType.MESH
F32 = jnp.float32
BF16 = jnp.bfloat16
ORDER = (
    ("ag", 0), ("ag", 1), ("ag", 2), ("ag", 3), ("mate",), ("s", 0), ("sp",), ("s", 1), ("cols",), ("near",),
    ("relay", 0), ("zi", 0, 0), ("relay", 1), ("zi", 0, 1), ("res", 0), ("relay", 2), ("res", 1), ("relay", 3),
    ("psend",), ("zi", 1, 0), ("res", 2), ("own",), ("zi", 1, 1), ("xc", 0, 0), ("xc", 0, 1), ("res", 3),
    ("pr1",), ("own1",), ("pr2",), ("first", 1), ("xc", 1, 0), ("xc", 1, 1), ("second", 1), ("first", 0),
    ("second", 0), ("fo", 0), ("first", 2), ("ph", 1), ("second", 2), ("own2",), ("tk", 1, 0), ("fo", 1),
    ("fh", 0, 0), ("tk", 1, 1), ("fh", 0, 1), ("ph", 0), ("ts", 0), ("ts", 1), ("tk", 0, 0), ("fh", 1, 0),
    ("tk", 0, 1), ("fh", 1, 1), ("tkeep",), ("ft", 0), ("ft", 1), ("fin",),
)


def dot(a, b):
    return jnp.dot(a, b, preferred_element_type=F32)


def twice_gelu(x):
    bent = x * (0.7978845608028654 + 0.035677408136300125 * (x * x))
    return (x + x * jnp.tanh(bent)).astype(BF16)


def fused_kernel(
    spans, pieces, cap, tokens_h, gain_h, w_ri_h, w_ro_h, w_ei_h, w_eo_h, expert_h, slot_h, gate_h, out,
    expert_v, slot_v, gate_v, gain, w_ri, w_ro, w_ei, w_eo, tok, res_hid, rows_raw, out_rows, out_rows2,
    own_table, hid, part, de_recv, pair_send, pair_recv, xf_send, xf_recv, zf_send, zf_recv,
    back, take, slot_gate, tpart, dt_recv, t_keep, xt_send, xt_recv, id_col, load_sem, send_sem, recv_sem,
):
    count, width = out.shape
    shards = tok.shape[1] // width
    padded = take.shape[2]
    hidden = res_hid.shape[1] - padded
    me = lax.axis_index("mp")
    z = lax.axis_index("expert")
    core = lax.rem(me, 2)
    chip = me // 2
    over = lax.rem(me + 2, 4)
    mate = me + 1 - 2 * core
    cross = lax.rem(mate + 2, 4)
    pair = z + 1 - 2 * lax.rem(z, 2)
    far = (lax.rem(z + 2, 4), 3 - z)
    to_over, to_mate, to_pair = {"mp": over}, {"mp": mate}, {"expert": pair}
    to_far = ({"expert": far[0]}, {"expert": far[1]})

    barrier = pltpu.get_barrier_semaphore()
    for dest in (to_over, to_mate, to_pair, to_far[0], to_far[1]):
        pl.semaphore_signal(barrier, inc=1, device_id=dest, device_id_type=MESH)

    def cols(shard):
        return pl.ds(pl.multiple_of(shard * width, width), width)

    loads = []
    for k, (src, dst) in enumerate((
        (expert_h, expert_v), (slot_h, slot_v), (tokens_h, tok.at[:, cols(me)]), (gate_h, gate_v), (gain_h, gain),
        (w_ri_h, w_ri), (w_ei_h.at[0], w_ei), (w_eo_h.at[0], w_eo), (w_ro_h, w_ro.at[:hidden]),
    )):
        load = pltpu.make_async_copy(src, dst, load_sem.at[k])
        load.start()
        loads.append(load)

    sent = []

    def send(src, dst, dest):
        k = len(sent)
        copy = pltpu.make_async_remote_copy(
            src_ref=src, dst_ref=dst, send_sem=send_sem.at[k], recv_sem=recv_sem.at[k],
            device_id=dest, device_id_type=MESH,
        )
        copy.start()
        sent.append(copy)
        return copy

    def pass_on(ref, dest):
        return send(ref, ref, dest)

    def send_table(e):
        base = (e * cap).astype(F32)
        return jnp.where(slot_rows + base == ids, 1.0, 0.0).astype(BF16)

    def chip_cols(j):
        block = chip if j == 0 else 1 - chip
        return pl.ds(pl.multiple_of(block * 2 * width, 2 * width), 2 * width)

    def first_layer(rows, w_ref):
        values = rows.astype(F32)
        mean = jnp.mean(values * values, axis=-1, keepdims=True)
        return twice_gelu(dot(rows, w_ref[...]) * lax.rsqrt(mean + 1e-05))

    with jax.named_scope("entry"):
        loads[0].wait()
        loads[1].wait()
        expert_row = expert_v[...].reshape(1, count)
        slot_row = slot_v[...].reshape(1, count)
        ids = jnp.where(slot_row >= 0, expert_row * cap + slot_row, -1).astype(F32)
        slot_rows = lax.broadcasted_iota(jnp.int32, (cap, count), 0).astype(F32)
        loads[2].wait()
    with jax.named_scope("barrier"):
        pl.semaphore_wait(barrier, 5)

    arrive = {}
    waited = set()

    def await_all(*names):
        for name in names:
            if name not in waited:
                waited.add(name)
                arrive[name].wait_recv()

    def tables():
        loads[3].wait()
        gate_row = gate_v[...].reshape(1, count)
        id_col[...] = jnp.broadcast_to(ids, (128, count)).T
        lane = lax.broadcasted_iota(jnp.int32, (count, 128), 1).astype(F32)
        for k, e in enumerate((pair, far[0], far[1], z)):
            base = (e * cap).astype(F32)
            gates = jnp.sum(jnp.where(slot_rows + base == ids, gate_row, 0.0), axis=1, keepdims=True)
            slot_gate[k] = jnp.broadcast_to(gates, (cap, 128))
            for lo in range(0, padded, 128):
                hit = jnp.where(lane + (base + lo) == id_col[...], 1.0, 0.0).astype(BF16)
                if k < 3:
                    take[k, :, lo:lo + 128] = hit
                else:
                    res_hid[:, hidden + lo:hidden + lo + 128] = hit
        back[:, cap:, :] = jnp.zeros((4, padded - cap, width), BF16)
        for k in range(4, 9):
            loads[k].wait()
        gain_col = jnp.broadcast_to(gain[...], (128, shards * width)).T
        for w_ref in (w_ri, w_ei):
            for lo in range(0, w_ref.shape[1], 128):
                w_ref[:, lo:lo + 128] = (w_ref[:, lo:lo + 128].astype(F32) * gain_col).astype(BF16)
        w_ro[hidden + cap:, :] = jnp.zeros((padded - cap, shards * width), BF16)

    def gated(rows, k):
        scale = slot_gate[k]
        return (rows * jnp.concatenate([scale] * (rows.shape[1] // 128), axis=1)).astype(BF16)

    lanes = tuple(slice(lo, lo + 128) for lo in range(0, width, 128))
    halves = (slice(0, count // 2), slice(count // 2, count))
    parts = range(len(pieces))

    def gather(h):
        arrive["over", h] = pass_on(tok.at[spans[h], cols(me)], to_over)

    def gather_mate():
        arrive["mate"] = pass_on(tok.at[:, cols(me)], to_mate)

    def far_send(f):
        out_rows[f + 1] = dot(send_table(far[f]), tok[:, cols(me)]).astype(BF16)
        for p, r in enumerate(pieces):
            arrive["z", f, p] = send(out_rows.at[f + 1, r], rows_raw.at[f + 1, r, cols(me)], to_far[f])

    def pair_send_own():
        out_rows[0] = dot(send_table(pair), tok[:, cols(me)]).astype(BF16)
        arrive["pair"] = send(out_rows.at[0], rows_raw.at[0, :, cols(me)], to_pair)

    def relay(h):
        await_all(("over", h))
        arrive["cross", h] = pass_on(tok.at[spans[h], cols(over)], to_mate)

    def residual(h):
        r = spans[h]
        await_all("mate", ("cross", h))
        res_hid[r, :hidden] = first_layer(tok[r], w_ri)

    def pair_send_over():
        out_rows2[...] = dot(send_table(pair), tok[:, cols(over)]).astype(BF16)
        arrive["pair2"] = send(out_rows2, rows_raw.at[0, :, cols(over)], to_pair)

    def far_in(f, p):
        await_all(("z", f, p))
        piece = rows_raw.at[f + 1, pieces[p], cols(me)]
        arrive["x", f, p] = pass_on(piece, to_over)
        arrive["near", f, p] = pass_on(piece, to_mate)

    def far_cross(f, p):
        await_all(("x", f, p))
        arrive["far", f, p] = pass_on(rows_raw.at[f + 1, pieces[p], cols(over)], to_mate)

    def pair_relay(k, s):
        await_all("pair2" if k else "pair")
        arrive["pairmate", k] = pass_on(rows_raw.at[0, :, cols(s)], to_mate)

    def expert_first(e):
        if e == 0:
            await_all(("pairmate", 0), ("pairmate", 1))
        else:
            await_all(*((kind, e - 1, p) for kind in ("near", "far") for p in parts))
        hid[e] = first_layer(rows_raw[e], w_ei)

    def expert_second(e):
        full = dot(hid[e], w_eo[...])
        for s in range(shards):
            part[e, s] = full[:, s * width:(s + 1) * width].astype(BF16)
        for j, s in ((1, cross), (0, mate)):
            arrive["part", j, e] = send(part.at[e, s], de_recv.at[j, e], to_mate)

    def chip_part(e, j, r):
        await_all(("part", j, e))
        return part[e, over if j else me, r].astype(F32) + de_recv[j, e, r].astype(F32)

    def own_rows(*shard_ids):
        for s in shard_ids:
            rows_raw[3, :, cols(s)] = dot(own_table[...], tok[:, cols(s)]).astype(BF16)

    def own_near():
        own_table[...] = send_table(z)
        await_all("mate")
        own_rows(me, mate)

    def own_first():
        own_rows(cross)
        hid[3] = first_layer(rows_raw[3], w_ei)

    def own_second():
        w_ro[hidden:hidden + cap, :] = gated(dot(hid[3], w_eo[...]), 3)

    def far_out(f):
        xf_send[f] = chip_part(f + 1, 1, slice(0, cap)).astype(BF16)
        for p, r in enumerate(pieces):
            arrive["xf", f, p] = send(xf_send.at[f, r], xf_recv.at[f, r], to_over)

    def far_home(f, p):
        r = pieces[p]
        own = chip_part(f + 1, 0, r)
        await_all(("xf", f, p))
        zf_send[f, r] = (own + xf_recv[f, r].astype(F32)).astype(BF16)
        arrive["zf", f, p] = send(zf_send.at[f, r], zf_recv.at[f, r], to_far[f])

    def pair_home(j):
        pair_send[j] = chip_part(0, j, slice(0, cap)).astype(BF16)
        for k, c in enumerate(lanes):
            arrive["back", j, k] = send(pair_send.at[j, :, c], pair_recv.at[j, :, c], to_pair)

    def token_part(j, i):
        r = halves[i]
        both = dot(res_hid[r], w_ro[:, chip_cols(j)])
        for c in range(2):
            tpart[j, c, r] = both[:, c * width:(c + 1) * width].astype(BF16)
        arrive["tok", j, i] = send(tpart.at[j, 1 - core, r], dt_recv.at[j, r], to_mate)

    def chip_sum(j, k):
        c = lanes[k]
        await_all(("tok", j, 0), ("tok", j, 1), ("back", j, k))
        back[j, :cap, c] = gated(pair_recv[j, :, c].astype(F32), 0)
        return dot(take[0], back[j, :, c]) + (tpart[j, core, :, c].astype(F32) + dt_recv[j, :, c].astype(F32))

    def token_send(k):
        c = lanes[k]
        xt_send[:, c] = chip_sum(1, k).astype(BF16)
        arrive["xt", k] = send(xt_send.at[:, c], xt_recv.at[:, c], to_over)

    def token_keep():
        for k, c in enumerate(lanes):
            t_keep[:, c] = chip_sum(0, k)

    def far_take(f):
        await_all(*(("zf", f, p) for p in parts))
        back[f + 2, :cap] = gated(zf_recv[f].astype(F32), f + 1)
        t_keep[...] = t_keep[...] + dot(take[f + 1], back[f + 2])

    def finish():
        for k, c in enumerate(lanes):
            await_all(("xt", k))
            out[:, c] = ((t_keep[:, c] + xt_recv[:, c].astype(F32)) * 0.5).astype(BF16)
        for copy in sent:
            copy.wait_send()

    steps = {
        "ag": gather, "mate": gather_mate, "s": far_send, "sp": pair_send_own, "cols": tables, "relay": relay,
        "res": residual, "psend": pair_send_over, "zi": far_in, "xc": far_cross, "own1": own_first, "near": own_near, "own": lambda: own_rows(over),
        "own2": own_second, "fo": far_out, "fh": far_home, "ph": pair_home, "tk": token_part, "ts": token_send,
        "tkeep": token_keep, "ft": far_take, "fin": finish, "first": expert_first, "second": expert_second,
        "pr1": lambda: pair_relay(0, me), "pr2": lambda: pair_relay(1, over),
    }
    for step in ORDER:
        with jax.named_scope("".join(map(str, step))):
            steps[step[0]](*step[1:])


def split_rows(rows, parts):
    step = -(-rows // (16 * parts)) * 16
    return tuple(slice(lo, min(lo + step, rows)) for lo in range(0, rows, step))


def fused(tokens, gain, w_res_in, w_res_out, w_exp_in, w_exp_out, expert_of, slot_of, gate_prob):
    count, width = tokens.shape
    shards = lax.axis_size("mp")
    experts = lax.axis_size("expert")
    cap = max(2, 5 * count // (4 * experts))
    padded = -(-cap // 128) * 128
    model, hidden = w_res_in.shape
    exp_hidden = w_exp_in.shape[2]
    vmem, hbm = pl.BlockSpec(memory_space=pltpu.VMEM), pl.BlockSpec(memory_space=pltpu.HBM)
    buf = lambda *shape: pltpu.VMEM(shape, BF16)
    wide = lambda *shape: pltpu.VMEM(shape, F32)
    spans, pieces = split_rows(count, 4), split_rows(cap, 2)
    copies = 15 + 3 * (width // 128) + 2 * len(spans) + 12 * len(pieces)
    args = (
        tokens, gain[None, :], w_res_in, w_res_out, w_exp_in, w_exp_out, expert_of, slot_of, gate_prob,
    )
    return pl.pallas_call(
        functools.partial(fused_kernel, spans, pieces, cap),
        out_shape=jax.ShapeDtypeStruct((count, width), BF16),
        in_specs=[hbm] * len(args),
        out_specs=vmem,
        scratch_shapes=[
            pltpu.VMEM((count,), jnp.int32), pltpu.VMEM((count,), jnp.int32), wide(count), wide(1, model),
            buf(model, hidden), buf(hidden + padded, model), buf(model, exp_hidden), buf(exp_hidden, model),
            buf(count, model), buf(count, hidden + padded),
            buf(4, cap, model), buf(3, cap, width), buf(cap, width),
            buf(cap, count), buf(4, cap, exp_hidden),
            buf(3, shards, cap, width), buf(2, 3, cap, width),
            buf(2, cap, width), buf(2, cap, width), buf(2, cap, width), buf(2, cap, width),
            buf(2, cap, width), buf(2, cap, width),
            buf(4, padded, width), buf(3, count, padded), wide(4, cap, 128),
            buf(2, 2, count, width), buf(2, count, width), wide(count, width),
            buf(count, width), buf(count, width), wide(count, 128),
            pltpu.SemaphoreType.DMA((9,)), pltpu.SemaphoreType.DMA((copies,)), pltpu.SemaphoreType.DMA((copies,)),
        ],
        name="fused_layer",
        compiler_params=pltpu.CompilerParams(
            collective_id=0, has_side_effects=True, vmem_limit_bytes=50 * 1024 * 1024
        ),
    )(*(pltpu.with_memory_space_constraint(a, pltpu.HBM) for a in args))


def pick(mesh):
    if mesh.shape["mp"] == 4 and mesh.shape["expert"] == 4:
        return fused
    return per_device


def solution(mesh):
    return jax.shard_map(
        pick(mesh),
        mesh=mesh,
        in_specs=(
            P(("groups", "expert"), "mp"),
            P(),
            P(None, "mp"),
            P("mp", None),
            P("expert", None, "mp"),
            P("expert", "mp", None),
            P(("groups", "expert")),
            P(("groups", "expert")),
            P(("groups", "expert")),
        ),
        out_specs=P(("groups", "expert"), "mp"),
        check_vma=False,
    )
```

```python
import functools

import jax
import jax.numpy as jnp
from jax import lax
from jax.experimental import pallas as pl
from jax.experimental.pallas import tpu as pltpu
from jax.sharding import PartitionSpec as P


def rms_rows(tokens, gain):
    values = tokens.astype(jnp.float32)
    inverse = lax.rsqrt(jnp.mean(values * values, axis=-1, keepdims=True) + 1e-05)
    return (values * inverse * gain).astype(jnp.bfloat16)


def per_device(
    tokens, gain, w_res_in, w_res_out, w_exp_in, w_exp_out, expert_of, slot_of, gate_prob
):
    full_rows = lax.all_gather(tokens, "mp", axis=1, tiled=True)
    normed = rms_rows(full_rows, gain)
    res_hidden = jax.nn.gelu(jnp.dot(normed, w_res_in, preferred_element_type=jnp.float32)).astype(
        jnp.bfloat16
    )
    res_part = jnp.dot(res_hidden, w_res_out, preferred_element_type=jnp.float32)
    row_count = expert_of.shape[0]
    experts = lax.axis_size("expert")
    capacity = max(2, 5 * row_count // (4 * experts))
    feat_width = tokens.shape[1]
    slot_id = jnp.where(slot_of >= 0, expert_of * capacity + slot_of, -1)
    slot_index = jnp.arange(experts * capacity, dtype=jnp.int32)
    send_table = (slot_index[:, None] == slot_id[None, :]).astype(jnp.bfloat16)
    take_table = (slot_id[:, None] == slot_index[None, :]).astype(jnp.bfloat16)
    local_in = w_exp_in[0]
    local_out = w_exp_out[0]
    mp_index = lax.axis_index("mp")
    own_slice = lax.dynamic_slice_in_dim(normed, mp_index * feat_width, feat_width, 1)
    outgoing = jnp.dot(send_table, own_slice, preferred_element_type=jnp.float32).astype(
        jnp.bfloat16
    )
    incoming = lax.all_to_all(
        outgoing.reshape(experts, capacity, feat_width),
        "expert",
        split_axis=0,
        concat_axis=0,
        tiled=True,
    )
    piece = lax.all_gather(incoming, "mp", axis=2, tiled=True)
    flat_piece = piece.reshape(-1, piece.shape[2])
    preact = jnp.dot(flat_piece, local_in, preferred_element_type=jnp.float32)
    exp_hidden = jax.nn.gelu(preact).astype(jnp.bfloat16)
    exp_part = jnp.dot(exp_hidden, local_out, preferred_element_type=jnp.float32)
    gate_column = gate_prob[:, None]
    summed = lax.psum_scatter(exp_part.astype(jnp.bfloat16), "mp", scatter_dimension=1, tiled=True)
    returned = lax.all_to_all(
        summed.reshape(experts, capacity, feat_width),
        "expert",
        split_axis=0,
        concat_axis=0,
        tiled=True,
    )
    moe_value = jnp.dot(
        take_table,
        returned.reshape(experts * capacity, feat_width),
        preferred_element_type=jnp.float32,
    )
    res_sum = lax.psum_scatter(
        res_part.astype(jnp.bfloat16), "mp", scatter_dimension=1, tiled=True
    ).astype(jnp.float32)
    return (res_sum + gate_column * moe_value).astype(jnp.bfloat16)


MESH = pl.DeviceIdType.MESH
F32 = jnp.float32
BF16 = jnp.bfloat16
ORDER = (
    ("ag", 0), ("ag", 1), ("ag", 2), ("ag", 3), ("mate",), ("s", 0), ("sp",), ("s", 1), ("cols",), ("near",),
    ("relay", 0), ("zi", 0, 0), ("relay", 1), ("zi", 0, 1), ("res", 0), ("relay", 2), ("res", 1), ("relay", 3),
    ("psend",), ("zi", 1, 0), ("res", 2), ("own",), ("zi", 1, 1), ("xc", 0, 0), ("xc", 0, 1), ("res", 3),
    ("pr1",), ("own1",), ("pr2",), ("first", 1), ("xc", 1, 0), ("xc", 1, 1), ("second", 1), ("first", 0),
    ("second", 0), ("fo", 0), ("first", 2), ("ph", 1), ("second", 2), ("own2",), ("tk", 1, 0), ("fo", 1),
    ("fh", 0, 0), ("tk", 1, 1), ("fh", 0, 1), ("ph", 0), ("ts", 0), ("ts", 1), ("tk", 0, 0), ("fh", 1, 0),
    ("tk", 0, 1), ("fh", 1, 1), ("tkeep",), ("ft", 0), ("ft", 1), ("fin",),
)


def dot(a, b):
    return jnp.dot(a, b, preferred_element_type=F32)


def twice_gelu(x):
    bent = x * (0.7978845608028654 + 0.035677408136300125 * (x * x))
    return (x + x * jnp.tanh(bent)).astype(BF16)


def fused_kernel(
    spans, pieces, cap, tokens_h, gain_h, w_ri_h, w_ro_h, w_ei_h, w_eo_h, expert_h, slot_h, gate_h, out,
    expert_v, slot_v, gate_v, gain, w_ri, w_ro, w_ei, w_eo, tok, res_hid, rows_raw, out_rows, out_rows2,
    own_table, hid, part, de_recv, pair_send, pair_recv, xf_send, xf_recv, zf_send, zf_recv,
    back, take, slot_gate, tpart, dt_recv, t_keep, xt_send, xt_recv, id_col, load_sem, send_sem, recv_sem,
):
    count, width = out.shape
    shards = tok.shape[1] // width
    padded = take.shape[2]
    hidden = res_hid.shape[1] - padded
    me = lax.axis_index("mp")
    z = lax.axis_index("expert")
    core = lax.rem(me, 2)
    chip = me // 2
    over = lax.rem(me + 2, 4)
    mate = me + 1 - 2 * core
    cross = lax.rem(mate + 2, 4)
    pair = z + 1 - 2 * lax.rem(z, 2)
    far = (lax.rem(z + 2, 4), 3 - z)
    to_over, to_mate, to_pair = {"mp": over}, {"mp": mate}, {"expert": pair}
    to_far = ({"expert": far[0]}, {"expert": far[1]})

    barrier = pltpu.get_barrier_semaphore()
    for dest in (to_over, to_mate, to_pair, to_far[0], to_far[1]):
        pl.semaphore_signal(barrier, inc=1, device_id=dest, device_id_type=MESH)

    def cols(shard):
        return pl.ds(pl.multiple_of(shard * width, width), width)

    loads = []
    for k, (src, dst) in enumerate((
        (expert_h, expert_v), (slot_h, slot_v), (tokens_h, tok.at[:, cols(me)]), (gate_h, gate_v), (gain_h, gain),
        (w_ri_h, w_ri), (w_ei_h.at[0], w_ei), (w_eo_h.at[0], w_eo), (w_ro_h, w_ro.at[:hidden]),
    )):
        load = pltpu.make_async_copy(src, dst, load_sem.at[k])
        load.start()
        loads.append(load)

    sent = []

    def send(src, dst, dest):
        k = len(sent)
        copy = pltpu.make_async_remote_copy(
            src_ref=src, dst_ref=dst, send_sem=send_sem.at[k], recv_sem=recv_sem.at[k],
            device_id=dest, device_id_type=MESH,
        )
        copy.start()
        sent.append(copy)
        return copy

    def pass_on(ref, dest):
        return send(ref, ref, dest)

    def send_table(e):
        base = (e * cap).astype(F32)
        return jnp.where(slot_rows + base == ids, 1.0, 0.0).astype(BF16)

    def chip_cols(j):
        block = chip if j == 0 else 1 - chip
        return pl.ds(pl.multiple_of(block * 2 * width, 2 * width), 2 * width)

    def first_layer(rows, w_ref):
        values = rows.astype(F32)
        mean = jnp.mean(values * values, axis=-1, keepdims=True)
        return twice_gelu(dot(rows, w_ref[...]) * lax.rsqrt(mean + 1e-05))

    with jax.named_scope("entry"):
        loads[0].wait()
        loads[1].wait()
        expert_row = expert_v[...].reshape(1, count)
        slot_row = slot_v[...].reshape(1, count)
        ids = jnp.where(slot_row >= 0, expert_row * cap + slot_row, -1).astype(F32)
        slot_rows = lax.broadcasted_iota(jnp.int32, (cap, count), 0).astype(F32)
        own_table[...] = send_table(far[0])
        loads[2].wait()
    with jax.named_scope("barrier"):
        pl.semaphore_wait(barrier, 5)

    arrive = {}
    waited = set()

    def await_all(*names):
        for name in names:
            if name not in waited:
                waited.add(name)
                arrive[name].wait_recv()

    def tables():
        loads[3].wait()
        gate_row = gate_v[...].reshape(1, count)
        id_col[...] = jnp.broadcast_to(ids, (128, count)).T
        lane = lax.broadcasted_iota(jnp.int32, (count, 128), 1).astype(F32)
        for k, e in enumerate((pair, far[0], far[1], z)):
            base = (e * cap).astype(F32)
            gates = jnp.sum(jnp.where(slot_rows + base == ids, gate_row, 0.0), axis=1, keepdims=True)
            slot_gate[k] = jnp.broadcast_to(gates, (cap, 128))
            for lo in range(0, padded, 128):
                hit = jnp.where(lane + (base + lo) == id_col[...], 1.0, 0.0).astype(BF16)
                if k < 3:
                    take[k, :, lo:lo + 128] = hit
                else:
                    res_hid[:, hidden + lo:hidden + lo + 128] = hit
        back[:, cap:, :] = jnp.zeros((4, padded - cap, width), BF16)
        for k in range(4, 9):
            loads[k].wait()
        gain_col = jnp.broadcast_to(gain[...], (128, shards * width)).T
        for w_ref in (w_ri, w_ei):
            for lo in range(0, w_ref.shape[1], 128):
                w_ref[:, lo:lo + 128] = (w_ref[:, lo:lo + 128].astype(F32) * gain_col).astype(BF16)
        w_ro[hidden + cap:, :] = jnp.zeros((padded - cap, shards * width), BF16)

    def gated(rows, k):
        scale = slot_gate[k]
        return (rows * jnp.concatenate([scale] * (rows.shape[1] // 128), axis=1)).astype(BF16)

    lanes = tuple(slice(lo, lo + 128) for lo in range(0, width, 128))
    halves = (slice(0, count // 2), slice(count // 2, count))
    parts = range(len(pieces))

    def gather(h):
        arrive["over", h] = pass_on(tok.at[spans[h], cols(me)], to_over)

    def gather_mate():
        arrive["mate"] = pass_on(tok.at[:, cols(me)], to_mate)

    def far_send(f):
        table = own_table[...] if f == 0 else send_table(far[f])
        out_rows[f + 1] = dot(table, tok[:, cols(me)]).astype(BF16)
        for p, r in enumerate(pieces):
            arrive["z", f, p] = send(out_rows.at[f + 1, r], rows_raw.at[f + 1, r, cols(me)], to_far[f])

    def pair_send_own():
        out_rows[0] = dot(send_table(pair), tok[:, cols(me)]).astype(BF16)
        arrive["pair"] = send(out_rows.at[0], rows_raw.at[0, :, cols(me)], to_pair)

    def relay(h):
        await_all(("over", h))
        arrive["cross", h] = pass_on(tok.at[spans[h], cols(over)], to_mate)

    def residual(h):
        r = spans[h]
        await_all("mate", ("cross", h))
        res_hid[r, :hidden] = first_layer(tok[r], w_ri)

    def pair_send_over():
        out_rows2[...] = dot(send_table(pair), tok[:, cols(over)]).astype(BF16)
        arrive["pair2"] = send(out_rows2, rows_raw.at[0, :, cols(over)], to_pair)

    def far_in(f, p):
        await_all(("z", f, p))
        piece = rows_raw.at[f + 1, pieces[p], cols(me)]
        arrive["x", f, p] = pass_on(piece, to_over)
        arrive["near", f, p] = pass_on(piece, to_mate)

    def far_cross(f, p):
        await_all(("x", f, p))
        arrive["far", f, p] = pass_on(rows_raw.at[f + 1, pieces[p], cols(over)], to_mate)

    def pair_relay(k, s):
        await_all("pair2" if k else "pair")
        arrive["pairmate", k] = pass_on(rows_raw.at[0, :, cols(s)], to_mate)

    def expert_first(e):
        if e == 0:
            await_all(("pairmate", 0), ("pairmate", 1))
        else:
            await_all(*((kind, e - 1, p) for kind in ("near", "far") for p in parts))
        hid[e] = first_layer(rows_raw[e], w_ei)

    def expert_second(e):
        full = dot(hid[e], w_eo[...])
        for s in range(shards):
            part[e, s] = full[:, s * width:(s + 1) * width].astype(BF16)
        for j, s in ((1, cross), (0, mate)):
            arrive["part", j, e] = send(part.at[e, s], de_recv.at[j, e], to_mate)

    def chip_part(e, j, r):
        await_all(("part", j, e))
        return part[e, over if j else me, r].astype(F32) + de_recv[j, e, r].astype(F32)

    def own_rows(*shard_ids):
        for s in shard_ids:
            rows_raw[3, :, cols(s)] = dot(own_table[...], tok[:, cols(s)]).astype(BF16)

    def own_near():
        own_table[...] = send_table(z)
        await_all("mate")
        own_rows(me, mate)

    def own_first():
        own_rows(cross)
        hid[3] = first_layer(rows_raw[3], w_ei)

    def own_second():
        w_ro[hidden:hidden + cap, :] = gated(dot(hid[3], w_eo[...]), 3)

    def far_out(f):
        xf_send[f] = chip_part(f + 1, 1, slice(0, cap)).astype(BF16)
        for p, r in enumerate(pieces):
            arrive["xf", f, p] = send(xf_send.at[f, r], xf_recv.at[f, r], to_over)

    def far_home(f, p):
        r = pieces[p]
        own = chip_part(f + 1, 0, r)
        await_all(("xf", f, p))
        zf_send[f, r] = (own + xf_recv[f, r].astype(F32)).astype(BF16)
        arrive["zf", f, p] = send(zf_send.at[f, r], zf_recv.at[f, r], to_far[f])

    def pair_home(j):
        pair_send[j] = chip_part(0, j, slice(0, cap)).astype(BF16)
        for k, c in enumerate(lanes):
            arrive["back", j, k] = send(pair_send.at[j, :, c], pair_recv.at[j, :, c], to_pair)

    def token_part(j, i):
        r = halves[i]
        both = dot(res_hid[r], w_ro[:, chip_cols(j)])
        for c in range(2):
            tpart[j, c, r] = both[:, c * width:(c + 1) * width].astype(BF16)
        arrive["tok", j, i] = send(tpart.at[j, 1 - core, r], dt_recv.at[j, r], to_mate)

    def chip_sum(j, k):
        c = lanes[k]
        await_all(("tok", j, 0), ("tok", j, 1), ("back", j, k))
        back[j, :cap, c] = gated(pair_recv[j, :, c].astype(F32), 0)
        return dot(take[0], back[j, :, c]) + (tpart[j, core, :, c].astype(F32) + dt_recv[j, :, c].astype(F32))

    def token_send(k):
        c = lanes[k]
        xt_send[:, c] = chip_sum(1, k).astype(BF16)
        arrive["xt", k] = send(xt_send.at[:, c], xt_recv.at[:, c], to_over)

    def token_keep():
        for k, c in enumerate(lanes):
            t_keep[:, c] = chip_sum(0, k)

    def far_take(f):
        await_all(*(("zf", f, p) for p in parts))
        back[f + 2, :cap] = gated(zf_recv[f].astype(F32), f + 1)
        t_keep[...] = t_keep[...] + dot(take[f + 1], back[f + 2])

    def finish():
        for k, c in enumerate(lanes):
            await_all(("xt", k))
            out[:, c] = ((t_keep[:, c] + xt_recv[:, c].astype(F32)) * 0.5).astype(BF16)
        for copy in sent:
            copy.wait_send()

    steps = {
        "ag": gather, "mate": gather_mate, "s": far_send, "sp": pair_send_own, "cols": tables, "relay": relay,
        "res": residual, "psend": pair_send_over, "zi": far_in, "xc": far_cross, "own1": own_first, "near": own_near, "own": lambda: own_rows(over),
        "own2": own_second, "fo": far_out, "fh": far_home, "ph": pair_home, "tk": token_part, "ts": token_send,
        "tkeep": token_keep, "ft": far_take, "fin": finish, "first": expert_first, "second": expert_second,
        "pr1": lambda: pair_relay(0, me), "pr2": lambda: pair_relay(1, over),
    }
    for step in ORDER:
        with jax.named_scope("".join(map(str, step))):
            steps[step[0]](*step[1:])


def split_rows(rows, parts):
    step = -(-rows // (16 * parts)) * 16
    return tuple(slice(lo, min(lo + step, rows)) for lo in range(0, rows, step))


def fused(tokens, gain, w_res_in, w_res_out, w_exp_in, w_exp_out, expert_of, slot_of, gate_prob):
    count, width = tokens.shape
    shards = lax.axis_size("mp")
    experts = lax.axis_size("expert")
    cap = max(2, 5 * count // (4 * experts))
    padded = -(-cap // 128) * 128
    model, hidden = w_res_in.shape
    exp_hidden = w_exp_in.shape[2]
    vmem, hbm = pl.BlockSpec(memory_space=pltpu.VMEM), pl.BlockSpec(memory_space=pltpu.HBM)
    buf = lambda *shape: pltpu.VMEM(shape, BF16)
    wide = lambda *shape: pltpu.VMEM(shape, F32)
    spans, pieces = split_rows(count, 4), split_rows(cap, 2)
    copies = 15 + 3 * (width // 128) + 2 * len(spans) + 12 * len(pieces)
    args = (
        tokens, gain[None, :], w_res_in, w_res_out, w_exp_in, w_exp_out, expert_of, slot_of, gate_prob,
    )
    return pl.pallas_call(
        functools.partial(fused_kernel, spans, pieces, cap),
        out_shape=jax.ShapeDtypeStruct((count, width), BF16),
        in_specs=[hbm] * len(args),
        out_specs=vmem,
        scratch_shapes=[
            pltpu.VMEM((count,), jnp.int32), pltpu.VMEM((count,), jnp.int32), wide(count), wide(1, model),
            buf(model, hidden), buf(hidden + padded, model), buf(model, exp_hidden), buf(exp_hidden, model),
            buf(count, model), buf(count, hidden + padded),
            buf(4, cap, model), buf(3, cap, width), buf(cap, width),
            buf(cap, count), buf(4, cap, exp_hidden),
            buf(3, shards, cap, width), buf(2, 3, cap, width),
            buf(2, cap, width), buf(2, cap, width), buf(2, cap, width), buf(2, cap, width),
            buf(2, cap, width), buf(2, cap, width),
            buf(4, padded, width), buf(3, count, padded), wide(4, cap, 128),
            buf(2, 2, count, width), buf(2, count, width), wide(count, width),
            buf(count, width), buf(count, width), wide(count, 128),
            pltpu.SemaphoreType.DMA((9,)), pltpu.SemaphoreType.DMA((copies,)), pltpu.SemaphoreType.DMA((copies,)),
        ],
        name="fused_layer",
        compiler_params=pltpu.CompilerParams(
            collective_id=0, has_side_effects=True, vmem_limit_bytes=50 * 1024 * 1024
        ),
    )(*(pltpu.with_memory_space_constraint(a, pltpu.HBM) for a in args))


def pick(mesh):
    if mesh.shape["mp"] == 4 and mesh.shape["expert"] == 4:
        return fused
    return per_device


def solution(mesh):
    return jax.shard_map(
        pick(mesh),
        mesh=mesh,
        in_specs=(
            P(("groups", "expert"), "mp"),
            P(),
            P(None, "mp"),
            P("mp", None),
            P("expert", None, "mp"),
            P("expert", "mp", None),
            P(("groups", "expert")),
            P(("groups", "expert")),
            P(("groups", "expert")),
        ),
        out_specs=P(("groups", "expert"), "mp"),
        check_vma=False,
    )
```
